32 devices in a mesh: sp: 16 (over z, x, core), tp: 2 (over y).
Axes of the slice: x: 2, y: 2, z: 4, core: 2. Of those that a mesh axis runs over, the one named last changes fastest.
Arguments:
- activations: bfloat16 [2, 2048, 8192], P(None, 'sp', 'tp'), may hold values from -250 to 250
- norm_gain: bfloat16 [8192], P('tp'), may hold values from 0.5 to 1.5
- keep_bits: int32 [2, 2048, 1024], P(None, 'sp', 'tp'), may hold values from 0 to 255, as said below
- key_value_weight: bfloat16 [1024, 8192], P('sp', 'tp'), may hold values from -0.0625 to 0.0625
- queries: bfloat16 [2, 2048, 4096], P('tp', 'sp'), may hold values from -68 to 68
- segment: int32 [4096], replicated, may hold values from 0 to 15, never falling along the last dimension, each value on 1 to 512 neighbouring positions
- cotangent: bfloat16 [2, 2048, 4096], P('tp', 'sp'), may hold values from -12 to 12
Outputs:
- attended: bfloat16 [2, 2048, 4096], P('tp', 'sp')
- grad_queries: bfloat16 [2, 2048, 4096], P('tp', 'sp')
- grad_activations: bfloat16 [2, 2048, 8192], P(None, 'sp', 'tp')
- grad_weight: float32 [1024, 8192], P('sp', 'tp')
- grad_gain: float32 [8192], P('tp')
The draws below stay inside these ranges and needn't reach their ends.
Inputs may be any that keep to these rules, and one draw needn't show every extreme that they name: Bit j of keep_bits[a, b, w] is the keep flag of feature 8 w + j. segment numbers never fall along the sequence; each document covers 1 to 512 positions, and one covers exactly 512.
All inputs are finite; a program needn't handle non-finite values.
Results may differ from the reference program's by a relative error of at most 0.012.
The reference program's roundings to bfloat16 on the way count: a program that leaves them out, or rounds other values in their place, can miss the bound.
Values may be sent and summed in bfloat16 or wider, within the bound.
A program may use at most 128 MiB of HBM per device.

```python
import math
import jax
import jax.numpy as jnp
import numpy as np
from jax import lax

D = 8192
HQ = 32
KVH = 4
HD = 128
DOC = 512
GROUP = 8
KVC = 1024
BLOCKS = 2
BROWS = 2048
SEQ = 4096


def draw_activations(key, part):
    subkeys = jax.random.split(jax.random.fold_in(key, 11), 3)
    slope_axis = jnp.linspace(0.0, 1.0, D, dtype=jnp.float32)
    values = jnp.clip(jax.random.normal(subkeys[0], (BLOCKS, BROWS, D), jnp.float32), -4.0, 4.0)
    columns = jnp.exp(jnp.log(3.0) * slope_axis + jax.random.uniform(subkeys[1], (D,), jnp.float32, jnp.log(0.5), jnp.log(2.0)))
    row_scale = jnp.exp(jax.random.uniform(subkeys[2], (BLOCKS, BROWS, 1), jnp.float32, 0.0, jnp.log(10.0)))
    return jnp.clip(values * columns * row_scale * 0.5, -250.0, 250.0).astype(jnp.bfloat16)


def draw_keep_bits(key, part):
    packed = jnp.zeros((BLOCKS, BROWS, D // 8), jnp.int32)
    for bit_index in range(8):
        digits = jax.random.randint(jax.random.fold_in(key, 50 + bit_index), (BLOCKS, BROWS, D // 8), 0, 10)
        packed = packed + jnp.left_shift((digits < 9).astype(jnp.int32), bit_index)
    return packed


def draw_queries(key, part):
    subkeys = jax.random.split(jax.random.fold_in(key, 23), 1)
    shape_full = (BLOCKS, BROWS, HQ * HD)
    values = jnp.clip(jax.random.normal(subkeys[0], shape_full, jnp.float32), -4.0, 4.0)
    return values.astype(jnp.bfloat16)


def draw_cotangent(key, part):
    subkeys = jax.random.split(jax.random.fold_in(key, 37), 2)
    shape_full = (BLOCKS, BROWS, HQ * HD)
    position = jnp.linspace(0.0, 1.0, BROWS, dtype=jnp.float32)[None, :, None]
    columns = jnp.exp(jax.random.uniform(subkeys[1], (1, 1, HQ * HD), jnp.float32, jnp.log(0.5), jnp.log(2.0)))
    values = jnp.clip(jax.random.normal(subkeys[0], shape_full, jnp.float32), -4.0, 4.0) * jnp.exp(jnp.log(3.0) * position)
    return jnp.clip(values * columns * 0.5, -12.0, 12.0).astype(jnp.bfloat16)


def block_scale(stream_key, extent, shards, least, high):
    factor_of = 1.0
    for dim, parts in shards:
        steps = jax.random.uniform(jax.random.fold_in(jax.random.fold_in(stream_key, 6), dim), (parts,), jnp.float32, least / len(shards), high / len(shards))
        factor_of = factor_of * jnp.repeat(jnp.exp(steps), extent[dim] // parts).reshape((-1,) + (1,) * (len(extent) - 1 - dim))
    return factor_of


def profile(number_of, total, bound, skew):
    portions = [(1 << 20) // math.isqrt(rank ** skew) + 1 for rank in range(2, number_of + 1)]
    rest, holding = total - bound - (number_of - 1), [1] * (number_of - 1)
    while rest > 0:
        movable = [i for i in range(number_of - 1) if holding[i] < bound]
        pool, left = sum([portions[i] for i in movable]), rest
        for i in movable:
            addition = min(bound - holding[i], max(1, left * portions[i] // pool), rest)
            holding[i] = holding[i] + addition
            rest = rest - addition
    return np.array([bound] + holding)


def ragged_sizes(own_key, number_of, total, bound, lean):
    if number_of == 2:
        one = jax.random.randint(own_key, (), max(1, total - bound), min(bound, total - 1) + 1)
        return jnp.stack([one, total - one])
    lengths = jnp.asarray(profile(number_of, total, bound, lean), jnp.int32)
    twos = (number_of - 1) // 2
    giver, sink = lengths[1:1 + 2 * twos:2], lengths[2:2 + 2 * twos:2]
    slack = jnp.minimum(giver - 1, bound - sink)
    shifted = jax.random.randint(jax.random.fold_in(own_key, 1), (twos,), 0, 1 << 20) % (slack + 1)
    lengths = lengths.at[1:1 + 2 * twos:2].set(giver - shifted).at[2:2 + 2 * twos:2].set(sink + shifted)
    return lengths[jax.random.permutation(jax.random.fold_in(own_key, 2), number_of)]


def bell_draw(own_key, extent, deviation, limit, cuts=(), kind=jnp.bfloat16):
    level = block_scale(own_key, extent, cuts, -0.22, 0.18) if cuts else 1.0
    result = jax.random.normal(own_key, extent, jnp.float32) * deviation * level
    return jnp.minimum(jnp.maximum(result, -limit), limit).astype(kind)


def setup_inputs(seed: int = 0) -> dict:
    streams_of = jax.random.split(jax.random.key(seed), 8)
    return {
        "activations": draw_activations(jax.random.fold_in(streams_of[7], 71), 0),
        "norm_gain": jnp.clip(1.0 + 0.1 * jax.random.normal(streams_of[1], (D,), jnp.float32), 0.5, 1.5).astype(jnp.bfloat16),
        "keep_bits": draw_keep_bits(jax.random.fold_in(streams_of[7], 71), 0),
        "key_value_weight": bell_draw(streams_of[3], (KVC, D), D ** -0.5, 0.0625, ((0, 16), (1, 2))),
        "queries": draw_queries(jax.random.fold_in(streams_of[7], 71), 0),
        "segment": jnp.searchsorted(jnp.cumsum(ragged_sizes(streams_of[5], 2 * SEQ // DOC, SEQ, DOC, 2)), jnp.arange(SEQ), side="right").astype(jnp.int32),
        "cotangent": draw_cotangent(jax.random.fold_in(streams_of[7], 71), 0),
    }


EPS = 1e-05
KEEP_RATE = 0.9
MASKED_SCORE = -1e+30

def unpack_flags(words):
    shifts = jnp.arange(8, dtype=jnp.int32)
    flags = jnp.bitwise_and(jnp.right_shift(words[..., None], shifts), 1)
    return flags.reshape(words.shape[:-1] + (words.shape[-1] * 8,)).astype(jnp.float32)

def group_sum(per_head, group_size):
    row_count, head_count, width = per_head.shape
    summed = lax.optimization_barrier(jnp.sum(per_head.reshape(row_count, head_count // group_size, group_size, width), axis=2))
    return summed.reshape(row_count, head_count // group_size * width).astype(jnp.bfloat16)

def fold_heads(grad_window):
    rounded = lax.optimization_barrier(grad_window.astype(jnp.bfloat16)).astype(jnp.float32)
    return group_sum(rounded, GROUP)

def block_attention(query_block, pair_window, grad_block, allowed):
    score_scale = HD ** (-0.5)
    query_wide = query_block.astype(jnp.float32)
    key_part = pair_window[:, :, :HD].astype(jnp.float32)
    value_part = pair_window[:, :, HD:].astype(jnp.float32)
    grad_wide = grad_block.astype(jnp.float32)
    scores = jnp.einsum('qhd,khd->hqk', query_wide, key_part) * score_scale
    scores = jnp.where(allowed[None], scores, MASKED_SCORE)
    row_max = lax.optimization_barrier(jnp.max(scores, axis=2, keepdims=True))
    weights = jnp.exp(scores - row_max)
    probabilities = weights / lax.optimization_barrier(jnp.sum(weights, axis=2, keepdims=True))
    probs_low = probabilities.astype(jnp.bfloat16)
    probs_back = probs_low.astype(jnp.float32)
    attended = jnp.einsum('hqk,khd->qhd', probs_back, value_part).astype(jnp.bfloat16)
    grad_probs = jnp.einsum('qhd,khd->hqk', grad_wide, value_part)
    row_inner = lax.optimization_barrier(jnp.sum(probabilities * grad_probs, axis=2, keepdims=True))
    grad_scores = (probabilities * (grad_probs - row_inner)).astype(jnp.bfloat16).astype(jnp.float32)
    grad_query = (jnp.einsum('hqk,khd->qhd', grad_scores, key_part) * score_scale).astype(jnp.bfloat16)
    grad_keys = jnp.einsum('hqk,qhd->khd', grad_scores, query_wide) * score_scale
    grad_values = jnp.einsum('hqk,qhd->khd', probs_back, grad_wide)
    return (attended, grad_query, jnp.concatenate([grad_keys, grad_values], axis=2))

def reference(activations, norm_gain, keep_bits, key_value_weight, queries, segment, cotangent):
    gain_wide = norm_gain.astype(jnp.float32)

    def norm_block(inputs):
        row_block, word_block = inputs
        row_wide = row_block.astype(jnp.float32)
        inv_rms = lax.rsqrt(lax.optimization_barrier(jnp.mean(row_wide * row_wide, axis=1, keepdims=True)) + EPS)
        drop_scale = unpack_flags(word_block) / KEEP_RATE
        return ((row_wide * inv_rms * gain_wide * drop_scale).astype(jnp.bfloat16), inv_rms)
    normed, inv_all = lax.map(norm_block, (activations, keep_bits))
    normed_rows = normed.reshape(SEQ, D)
    projected = jnp.dot(normed_rows, key_value_weight.T, preferred_element_type=jnp.float32).astype(jnp.bfloat16)
    pair_heads = jnp.repeat(projected.reshape(SEQ, KVH, 2 * HD), GROUP, axis=1)
    pair_padded = jnp.concatenate([jnp.zeros((DOC, HQ, 2 * HD), jnp.bfloat16), pair_heads], axis=0)
    segment_padded = jnp.concatenate([jnp.full((DOC,), -1, jnp.int32), segment.astype(jnp.int32)])
    query_rows = queries.reshape(SEQ, HQ, HD)
    grad_rows = cotangent.reshape(SEQ, HQ, HD)
    causal = jnp.arange(2 * DOC, dtype=jnp.int32)[None, :] <= jnp.arange(DOC, dtype=jnp.int32)[:, None] + DOC

    def attend_step(pending, block_index):
        offset = (block_index * DOC).astype(jnp.int32)
        query_block = lax.dynamic_slice_in_dim(query_rows, offset, DOC, 0)
        grad_block = lax.dynamic_slice_in_dim(grad_rows, offset, DOC, 0)
        pair_window = lax.dynamic_slice_in_dim(pair_padded, offset, 2 * DOC, 0)
        seg_query = lax.dynamic_slice_in_dim(segment.astype(jnp.int32), offset, DOC, 0)
        seg_keys = lax.dynamic_slice_in_dim(segment_padded, offset, 2 * DOC, 0)
        allowed = causal & (seg_query[:, None] == seg_keys[None, :])
        attended, grad_query, grad_window = block_attention(query_block, pair_window, grad_block, allowed)
        finished = fold_heads(pending + grad_window[:DOC])
        return (grad_window[DOC:], (attended, grad_query, finished))
    final_tail, (outputs, query_grads, finished) = lax.scan(attend_step, jnp.zeros((DOC, HQ, 2 * HD), jnp.float32), jnp.arange(SEQ // DOC, dtype=jnp.int32))
    pair_grads = jnp.concatenate([finished[1:], fold_heads(final_tail)[None]], axis=0).reshape(SEQ, KVC)
    grad_weight = jnp.dot(pair_grads.T, normed_rows, preferred_element_type=jnp.float32) * SEQ ** (-0.5)

    def grad_block_norm(inputs):
        row_block, word_block, inv_rms, grad_pairs = inputs
        row_wide = row_block.astype(jnp.float32)
        drop_scale = unpack_flags(word_block) / KEEP_RATE
        hidden_grad = jnp.dot(grad_pairs, key_value_weight, preferred_element_type=jnp.float32)
        scaled = hidden_grad * drop_scale
        upstream = scaled * gain_wide
        row_dots = lax.optimization_barrier(jnp.sum(upstream * row_wide, axis=1, keepdims=True))
        grad_rows_out = (inv_rms * upstream - row_wide * (inv_rms * inv_rms * inv_rms) * row_dots / D).astype(jnp.bfloat16)
        gain_part = lax.optimization_barrier(jnp.sum(scaled * row_wide * inv_rms, axis=0))
        return (grad_rows_out, gain_part)
    grad_activations, gain_parts = lax.map(grad_block_norm, (activations, keep_bits, inv_all, pair_grads.reshape(BLOCKS, BROWS, KVC)))
    grad_gain = lax.optimization_barrier(jnp.sum(gain_parts, axis=0)) * SEQ ** (-0.5)
    attended = outputs.reshape(BLOCKS, BROWS, HQ * HD)
    grad_queries = query_grads.reshape(BLOCKS, BROWS, HQ * HD)
    return (attended, grad_queries, grad_activations, grad_weight, grad_gain)
```

```python
import functools

import jax
import jax.numpy as jnp
from jax import lax
from jax.experimental import pallas as pl
from jax.experimental.pallas import tpu as pltpu
from jax.sharding import PartitionSpec as P

D = 8192
HQ = 32
KVH = 4
HD = 128
DOC = 512
GROUP = 8


EPS = 1e-05
KEEP_RATE = 0.9
MASKED_SCORE = -1e30


BOTH = ("sp", "tp")


def shifted(block, distance):
    sp_size, tp_size = lax.axis_size("sp"), lax.axis_size("tp")
    places = range(tp_size * sp_size)
    device = [p % sp_size * tp_size + p // sp_size for p in places]
    route = [(device[p], device[p + distance]) for p in places if p + distance in places]
    return lax.ppermute(block, BOTH, route)


def unpack_flags(words):
    shifts = jnp.arange(8, dtype=jnp.int32)
    flags = jnp.bitwise_and(jnp.right_shift(words[..., None], shifts), 1)
    return flags.reshape(words.shape[:-1] + (words.shape[-1] * 8,)).astype(jnp.float32)


def attend_kernel(halo, seg_query_ref, seg_keys_ref, query_ref, grad_ref, *refs):
    pair_refs = refs[: halo + 1]
    attended_ref, grad_query_ref, rim_grad_ref, own_grad_ref, probs_all, scores_all = refs[halo + 1 :]
    score_scale = HD ** (-0.5)
    rows = query_ref.shape[0]
    keys = rows * (halo + 1)
    key_part = jnp.concatenate([r[:, :HD] for r in pair_refs], axis=0)
    value_part = jnp.concatenate([r[:, HD:] for r in pair_refs], axis=0)
    position = lax.broadcasted_iota(jnp.int32, (rows, keys), 0) + halo * rows
    other = lax.broadcasted_iota(jnp.int32, (rows, keys), 1)
    allowed = (other <= position) & (seg_query_ref[...] == seg_keys_ref[...])
    across = (((1,), (1,)), ((), ()))
    for n in range(GROUP):
        columns = slice(n * HD, (n + 1) * HD)
        query = query_ref[:, columns]
        grad = grad_ref[:, columns]
        scores = (
            lax.dot_general(query, key_part, across, preferred_element_type=jnp.float32)
            * score_scale
        )
        scores = jnp.where(allowed, scores, MASKED_SCORE)
        weights = jnp.exp(scores - jnp.max(scores, axis=1, keepdims=True))
        probabilities = weights / jnp.sum(weights, axis=1, keepdims=True)
        probs_low = probabilities.astype(jnp.bfloat16)
        attended_ref[:, columns] = jnp.dot(
            probs_low, value_part, preferred_element_type=jnp.float32
        ).astype(jnp.bfloat16)
        grad_probs = lax.dot_general(grad, value_part, across, preferred_element_type=jnp.float32)
        row_inner = jnp.sum(probabilities * grad_probs, axis=1, keepdims=True)
        grad_scores = (probabilities * (grad_probs - row_inner)).astype(jnp.bfloat16)
        grad_query_ref[:, columns] = (
            jnp.dot(grad_scores, key_part, preferred_element_type=jnp.float32) * score_scale
        ).astype(jnp.bfloat16)
        probs_all[n * rows : (n + 1) * rows, :] = probs_low
        scores_all[n * rows : (n + 1) * rows, :] = grad_scores
    down = (((0,), (0,)), ((), ()))
    query_stack = jnp.concatenate([query_ref[:, n * HD : (n + 1) * HD] for n in range(GROUP)], axis=0)
    grad_stack = jnp.concatenate([grad_ref[:, n * HD : (n + 1) * HD] for n in range(GROUP)], axis=0)
    grad_keys = (
        lax.dot_general(scores_all[...], query_stack, down, preferred_element_type=jnp.float32)
        * score_scale
    )
    grad_values = lax.dot_general(
        probs_all[...], grad_stack, down, preferred_element_type=jnp.float32
    )
    edge = halo * rows
    rim_grad_ref[:, :HD] = grad_keys[:edge].astype(jnp.bfloat16)
    rim_grad_ref[:, HD:] = grad_values[:edge].astype(jnp.bfloat16)
    own_grad_ref[:, :HD] = grad_keys[edge:]
    own_grad_ref[:, HD:] = grad_values[edge:]


def attend(queries, cotangent, pairs, seg_query, seg_keys):
    halo = len(pairs) - 1
    rows = queries.shape[0]
    keys = rows * (halo + 1)
    wide = GROUP * HD
    whole = lambda shape: pl.BlockSpec(shape, lambda g: (0, 0))
    group = lambda shape: pl.BlockSpec(shape, lambda g: (0, g))
    return pl.pallas_call(
        functools.partial(attend_kernel, halo),
        grid=(KVH,),
        in_specs=[whole((rows, 1)), whole((1, keys)), group((rows, wide)), group((rows, wide))]
        + [group((rows, 2 * HD))] * (halo + 1),
        out_specs=[
            group((rows, wide)),
            group((rows, wide)),
            group((halo * rows, 2 * HD)),
            group((rows, 2 * HD)),
        ],
        out_shape=[
            jax.ShapeDtypeStruct(queries.shape, jnp.bfloat16),
            jax.ShapeDtypeStruct(queries.shape, jnp.bfloat16),
            jax.ShapeDtypeStruct((halo * rows, KVH * 2 * HD), jnp.bfloat16),
            jax.ShapeDtypeStruct((rows, KVH * 2 * HD), jnp.float32),
        ],
        scratch_shapes=[
            pltpu.VMEM((GROUP * rows, keys), jnp.bfloat16),
            pltpu.VMEM((GROUP * rows, keys), jnp.bfloat16),
        ],
        cost_estimate=pl.CostEstimate(
            flops=10 * HQ * rows * keys * HD, bytes_accessed=8 * rows * HQ * HD, transcendentals=HQ * rows * keys
        ),
        compiler_params=pltpu.CompilerParams(vmem_limit_bytes=40 * 2**20),
    )(seg_query[:, None], seg_keys[None, :], queries, cotangent, *pairs)


def on_device(activations, norm_gain, keep_bits, key_value_weight, queries, segment, cotangent):
    sp_size = lax.axis_size("sp")
    tp_size = lax.axis_size("tp")
    tp_index = lax.axis_index("tp")
    block_count, row_count, local_width = activations.shape
    seq_length = row_count * sp_size * tp_size
    gain_wide = norm_gain.astype(jnp.float32)
    input_wide = activations.astype(jnp.float32)
    square_total = lax.psum(jnp.sum(input_wide * input_wide, axis=2), "tp")
    inv_rms = lax.rsqrt(square_total[..., None] / D + EPS)
    drop_scale = unpack_flags(keep_bits) / KEEP_RATE
    normed = (input_wide * inv_rms * gain_wide * drop_scale).astype(jnp.bfloat16)
    weight_full = lax.all_gather(key_value_weight, "sp", axis=0, tiled=True)
    pair_tokens = lax.psum_scatter(
        jnp.einsum("arf,cf->arc", normed, weight_full, preferred_element_type=jnp.float32),
        "tp",
        scatter_dimension=0,
        tiled=True,
    )[0].astype(jnp.bfloat16)
    place = tp_index * sp_size + lax.axis_index("sp")
    halo = -(-(DOC - 1) // row_count)
    pairs = [shifted(pair_tokens, d) for d in range(halo, 0, -1)] + [pair_tokens]
    segment_padded = jnp.concatenate([jnp.full((halo * row_count,), -1, jnp.int32), segment])
    segment_keys = lax.dynamic_slice_in_dim(
        segment_padded, place * row_count, (halo + 1) * row_count, 0
    )
    segment_query = segment_keys[halo * row_count :]
    attended, grad_queries, rim_grad, own_grad = attend(
        queries[0], cotangent[0], pairs, segment_query, segment_keys
    )
    for d in range(halo, 0, -1):
        part = rim_grad[(halo - d) * row_count : (halo - d + 1) * row_count]
        own_grad = own_grad + shifted(part, -d).astype(jnp.float32)
    pair_grad_rows = own_grad.astype(jnp.bfloat16)
    pair_grad_all = lax.all_gather(pair_grad_rows[None], "tp", axis=0, tiled=True)
    hidden_grad = jnp.einsum(
        "arc,cf->arf", pair_grad_all, weight_full, preferred_element_type=jnp.float32
    )
    grad_weight = lax.psum_scatter(
        jnp.einsum(
            "arc,arf->cf", pair_grad_all, normed, preferred_element_type=jnp.float32
        ).astype(jnp.bfloat16),
        "sp",
        scatter_dimension=0,
        tiled=True,
    ).astype(jnp.float32) * seq_length ** (-0.5)
    scaled = hidden_grad * drop_scale
    upstream = scaled * gain_wide
    row_dots = lax.psum(jnp.sum(upstream * input_wide, axis=2), "tp")[..., None]
    grad_activations = (
        inv_rms * upstream - input_wide * (inv_rms * inv_rms * inv_rms) * row_dots / D
    ).astype(jnp.bfloat16)
    gain_local = jnp.sum(scaled * input_wide * inv_rms, axis=(0, 1))
    grad_gain = lax.psum(gain_local, "sp") * seq_length ** (-0.5)
    return (attended[None], grad_queries[None], grad_activations, grad_weight, grad_gain)


def solution(mesh):
    return jax.shard_map(
        on_device,
        mesh=mesh,
        in_specs=(
            P(None, "sp", "tp"),
            P("tp"),
            P(None, "sp", "tp"),
            P("sp", "tp"),
            P("tp", "sp", None),
            P(),
            P("tp", "sp", None),
        ),
        out_specs=(
            P("tp", "sp", None),
            P("tp", "sp", None),
            P(None, "sp", "tp"),
            P("sp", "tp"),
            P("tp"),
        ),
        check_vma=False,
    )
```
